32 devices in a mesh: seq: 8 (over y, x, core), sub: 4 (over z).
Axes of the slice: x: 2, y: 2, z: 4, core: 2. Of those that a mesh axis runs over, the one named last changes fastest.
Arguments:
- tokens: bfloat16 [2048, 4096], P('seq'), may hold values from -6 to 6
- w_split: bfloat16 [4096, 4096], P(None, 'sub'), may hold values from -0.09375 to 0.09375
- w_merge: bfloat16 [4096, 4096], P('sub'), may hold values from -0.09375 to 0.09375
- expert_in: bfloat16 [32, 1024, 2048], P(('seq', 'sub')), may hold values from -0.1875 to 0.1875
- expert_out: bfloat16 [32, 1024, 1024], P(('seq', 'sub')), may hold values from -0.1875 to 0.1875
- expert_ids: int32 [4, 2048, 2], P('sub', 'seq'), may hold values from 0 to 31, all different within a row; in each aligned block of 256 rows (0 to 255, 256 to 511, ..., all dimensions but the last counted through in order) at most 24 rows name the same one
- combine_q: int32 [4, 2048, 2], P('sub', 'seq'), may hold values from 4096 to 65536
- capacity: int32 [32], replicated, may hold values from 12 to 24
Outputs:
- mixed: bfloat16 [2048, 4096], P('seq', 'sub')
The draws below stay inside these ranges and needn't reach their ends.
Inputs may be any that keep to these rules, and one draw needn't show every extreme that they name: `expert_ids`: in each block of 256 positions of one sub-head, the ids of a position differ, no expert is named more than 24 times, a bound that some block reaches.
All inputs are finite; a program needn't handle non-finite values.
Results may differ from the reference program's by a relative error of at most 0.0076.
Values may be sent and summed in bfloat16 or wider, within the bound.
A program may use at most 128 MiB of HBM per device.

```python
import math
import jax
import jax.numpy as jnp
import numpy as np
from jax import lax

D = 4096
HEADS = 4
FFE = 1024
TOPK = 2
TOK_DEV = 256
SUBW = 1024
EXPERTS = 32
CAP = 24
TOKENS = 2048
N_SEQ = 8


def with_ends(entries, rng, smallest, high):
    longest = entries.shape.index(max(entries.shape))
    spots = []
    for shift in (0, 1):
        where = [jax.random.randint(jax.random.fold_in(rng, axis), (), 0, length) for axis, length in enumerate(entries.shape)]
        where[longest] = (where[longest] + shift) % entries.shape[longest]
        spots.append(tuple(where))
    return entries.at[spots[0]].set(smallest).at[spots[1]].set(high)


def shard_levels(key, extent, split, least, top_value):
    def one(axis_at, blocks):
        draws = jax.random.uniform(jax.random.fold_in(jax.random.fold_in(key, 6), axis_at), (blocks,), jnp.float32, least / len(split), top_value / len(split))
        return jnp.repeat(jnp.exp(draws), extent[axis_at] // blocks).reshape((-1,) + (1,) * (len(extent) - axis_at - 1))

    gain = one(*split[0])
    for cut in split[1:]:
        gain = gain * one(*cut)
    return gain


def deal_out(rng, own, number, rows, number_of, top, limit, lean):
    ranking = jax.random.permutation(rng, number_of)
    crowded, common = shares(number_of, rows * top, limit, lean, True), shares(number_of, rows * top, limit, lean, False)
    places = jnp.arange(number_of)

    def named(lengths, rotation):
        used = int((lengths > 0).sum())
        fixed = max(1, used // 4)
        moved = fixed + (places - fixed + rotation * (used - fixed)) % max(1, number_of - fixed)
        return jnp.zeros((number_of,), jnp.int32).at[ranking[jnp.where(places < fixed, places, moved)]].set(jnp.asarray(lengths, jnp.int32))

    lengths = jnp.where(number % 4 == 0, named(crowded, number // 4), named(common, number - number // 4 - 1))
    mixed = jax.random.permutation(jax.random.fold_in(own, 3), number_of)
    source_of, sink = mixed[0:number_of // 2 * 2:2], mixed[1:number_of // 2 * 2:2]
    slack = jnp.minimum(lengths[source_of] - 1, limit - lengths[sink]) // 2
    slack = jnp.where((source_of == ranking[0]) | (sink == ranking[0]) | (lengths[sink] == 0), 0, jnp.maximum(slack, 0))
    moved = jax.random.randint(jax.random.fold_in(own, 4), (number_of // 2,), 0, 1 << 20) % (slack + 1)
    lengths = lengths.at[source_of].add(-moved).at[sink].add(moved)
    members = jnp.searchsorted(jnp.cumsum(lengths), jnp.arange(rows * top), side="right").astype(jnp.int32)
    table = members.reshape(top, rows).T
    table = table[jax.random.permutation(jax.random.fold_in(own, 1), rows)]
    rotation = jax.random.randint(jax.random.fold_in(own, 2), (rows, 1), 0, top)
    return jnp.take_along_axis(table, (jnp.arange(top)[None, :] + rotation) % top, axis=1)


def shares(number_of, total, limit, slope, full):
    loads = [(1 << 20) // math.isqrt(rank ** slope) + 1 for rank in range(1, number_of + 1)]
    largest = limit if full else min(limit, max(-(-total // number_of), total * loads[0] // sum(loads)))
    least = 1 if total - largest >= number_of - 1 else 0
    counts, rest = [largest] + [least] * (number_of - 1), total - largest - least * (number_of - 1)
    while rest > 0:
        candidates = [i for i in range(1, number_of) if counts[i] < largest] or [i for i in range(1, number_of) if counts[i] < limit]
        mass, remaining = sum([loads[i] for i in candidates]), rest
        for i in candidates:
            addition = min(limit - counts[i], max(1, remaining * loads[i] // mass), rest)
            counts[i] = counts[i] + addition
            rest = rest - addition
    return np.array(counts)


def centred(key, shape, scale, bound, split=(), kind=jnp.bfloat16):
    array = scale * jax.random.normal(key, shape, jnp.float32)
    if split:
        array = array * shard_levels(key, shape, split, -0.22, 0.18)
    return jnp.clip(array, -bound, bound).astype(kind)


def setup_inputs(seed: int = 0) -> dict:
    key_of = jax.random.split(jax.random.key(seed), 9)
    tokens = centred(key_of[0], (TOKENS, D), 1.0, 6.0, ((0, 8),))
    w_split = centred(key_of[1], (D, D), D ** -0.5, 0.09375, ((1, 4),))
    w_merge = centred(key_of[2], (D, D), D ** -0.5, 0.09375, ((0, 4),))
    expert_in = centred(key_of[3], (EXPERTS, SUBW, 2 * FFE), SUBW ** -0.5, 0.1875, ((0, 32),))
    expert_out = centred(key_of[4], (EXPERTS, FFE, SUBW), FFE ** -0.5, 0.1875, ((0, 32),))
    expert_ids_keys = jax.random.split(jax.random.fold_in(key_of[5], 1), HEADS * TOKENS // TOK_DEV)
    expert_ids_turns = jax.random.permutation(jax.random.fold_in(key_of[5], 3), HEADS * TOKENS // TOK_DEV)
    expert_ids = jax.vmap(lambda own, number: deal_out(jax.random.fold_in(key_of[5], 2), own, number, TOK_DEV, EXPERTS, TOPK, CAP, 2))(expert_ids_keys, expert_ids_turns).reshape((HEADS, TOKENS, TOPK))
    combine_q = with_ends(jax.random.randint(key_of[6], (HEADS, TOKENS, TOPK), 4096, 65537), jax.random.fold_in(key_of[6], 1), 4096, 65536).astype(jnp.int32)
    capacity = with_ends(jax.random.randint(key_of[7], (EXPERTS,), CAP // 2, CAP + 1), jax.random.fold_in(key_of[7], 1), CAP // 2, CAP).astype(jnp.int32)
    return {"tokens": tokens, "w_split": w_split, "w_merge": w_merge, "expert_in": expert_in, "expert_out": expert_out, "expert_ids": expert_ids, "combine_q": combine_q, "capacity": capacity}


def expert_ffn(inputs, w_in, w_out):
    gate_up = jnp.dot(inputs, w_in, preferred_element_type=jnp.float32)
    ffe_width = w_out.shape[0]
    hidden = (jax.nn.silu(gate_up[:, :ffe_width]) * gate_up[:, ffe_width:]).astype(jnp.bfloat16)
    return jnp.dot(hidden, w_out, preferred_element_type=jnp.float32).astype(jnp.bfloat16)


def reference(tokens, w_split, w_merge, expert_in, expert_out, expert_ids, combine_q, capacity):
    sub_tokens = jnp.dot(tokens, w_split, preferred_element_type=jnp.float32).astype(jnp.bfloat16)
    table = sub_tokens.reshape(TOKENS, HEADS, SUBW).transpose(1, 0, 2).reshape(HEADS * TOKENS, SUBW)
    block_count = HEADS * N_SEQ
    expert_of = expert_ids.reshape(block_count, TOPK * TOK_DEV)
    onehot = (expert_of[:, :, None] == jnp.arange(EXPERTS, dtype=jnp.int32)[None, None, :]).astype(jnp.int32)
    order_rank = jnp.sum((jnp.cumsum(onehot, axis=1) - onehot) * onehot, axis=2)
    cap_limit = jnp.sum(onehot * capacity[None, None, :], axis=2)
    is_kept = order_rank < cap_limit
    block_id = jnp.arange(block_count, dtype=jnp.int32)[:, None]
    slot_index = (expert_of * block_count + block_id) * CAP + order_rank
    total_slots = EXPERTS * block_count * CAP
    slot_index = jnp.where(is_kept, slot_index, total_slots)
    entry_pos = jnp.arange(TOPK * TOK_DEV, dtype=jnp.int32)[None, :]
    row_index = block_id * TOK_DEV + entry_pos // TOPK
    weights = combine_q.reshape(block_count, TOPK * TOK_DEV).astype(jnp.float32) / 65536.0
    slot_row = jnp.full((total_slots,), -1, jnp.int32).at[slot_index.reshape(-1)].set(
        jnp.broadcast_to(row_index, slot_index.shape).reshape(-1), mode="drop")
    slot_weight = jnp.zeros((total_slots,), jnp.float32).at[slot_index.reshape(-1)].set(
        weights.reshape(-1), mode="drop")
    slot_row = slot_row.reshape(EXPERTS, block_count * CAP)
    slot_weight = slot_weight.reshape(EXPERTS, block_count * CAP)

    def one_expert(running, inputs_e):
        rows_here, weights_here, w_in, w_out = inputs_e
        is_valid = rows_here >= 0
        safe_row = jnp.maximum(rows_here, 0)
        picked = jnp.where(is_valid[:, None], table[safe_row], jnp.zeros((), jnp.bfloat16))
        answer = expert_ffn(picked, w_in, w_out)
        weighted = jnp.where(is_valid[:, None], weights_here[:, None] * answer.astype(jnp.float32), jnp.zeros((), jnp.float32))
        return running.at[safe_row].add(weighted), None

    start = jnp.zeros((HEADS * TOKENS, SUBW), jnp.float32)
    running, _ = lax.scan(one_expert, start, (slot_row, slot_weight, expert_in, expert_out))
    head_out = running.astype(jnp.bfloat16).reshape(HEADS, TOKENS, SUBW).transpose(1, 0, 2).reshape(TOKENS, D)
    return jnp.dot(head_out, w_merge, preferred_element_type=jnp.float32).astype(jnp.bfloat16)
```

```python
import functools

import jax
import jax.numpy as jnp
from jax import lax
from jax.experimental import pallas as pl
from jax.experimental.pallas import tpu as pltpu
from jax.sharding import PartitionSpec as P

MESH = pl.DeviceIdType.MESH
TILE = 256
CHUNKS = 4
LAG = 2
VMEM_BYTES = 60 * 1024 * 1024
F32 = jnp.float32
BF16 = jnp.bfloat16


def layer_kernel(n_seq, n_sub, slots, route, capacity, tokens_hbm, w_split_hbm, w_in_hbm,
                 w_out_hbm, w_merge_hbm, out,
                 tokens, w_split, w_in, w_out, w_merge, info, mine, raw, pick, mix, packed,
                 received, x, hidden, answers, returned, part_out, part_in, acc, head,
                 sending, landed,
                 load_sem, info_send, info_recv, raw_send, raw_recv, slot_send, slot_recv,
                 ans_send, ans_recv, part_send, part_recv, hop_send, hop_recv):
    s, z = lax.axis_index("seq"), lax.axis_index("sub")
    half = n_sub // 2
    side = z // half
    q = jnp.where(side == 0, z, n_sub - 1 - z)
    inner = q == half - 1
    n = n_seq * n_sub
    peers = half * n_seq
    rows, width = acc.shape
    wide = width // CHUNKS
    fold_w = wide // 2
    ffe = w_out.shape[0]
    group = n_seq * slots

    def plane(where, depth):
        return jnp.where(where == 0, depth, n_sub - 1 - depth)

    def near(r, depth):
        return (lax.rem(s + r, n_seq), plane(side, depth))

    def across(depth):
        return (s, plane(1 - side, depth))

    fetch_tokens = pltpu.make_async_copy(tokens_hbm, tokens, load_sem.at[CHUNKS])
    fetch_in = pltpu.make_async_copy(w_in_hbm, w_in, load_sem.at[CHUNKS + 1])
    fetch_out = pltpu.make_async_copy(w_out_hbm, w_out, load_sem.at[CHUNKS + 2])
    fetch_merge = pltpu.make_async_copy(w_merge_hbm, w_merge, load_sem.at[CHUNKS + 3])

    def fetch_split(c):
        return pltpu.make_async_copy(
            w_split_hbm.at[:, pl.ds(c * wide, wide)], w_split.at[c], load_sem.at[c])

    fetch_tokens.start()
    for c in range(CHUNKS):
        fetch_split(c).start()

    barrier = pltpu.get_barrier_semaphore()
    for p in range(half):
        @pl.loop(0, n_seq)
        def _(r):
            @pl.when((r != 0) | (q != p))
            def _():
                pl.semaphore_signal(barrier, inc=1, device_id=near(r, p), device_id_type=MESH)

        @pl.when(inner | (p == half - 1))
        def _():
            pl.semaphore_signal(barrier, inc=1, device_id=across(p), device_id_type=MESH)

    def remote(src, dst, send, recv, to):
        return pltpu.make_async_remote_copy(src_ref=src, dst_ref=dst, send_sem=send,
                                            recv_sem=recv, device_id=to, device_id_type=MESH)

    def info_copy():
        return remote(route, info.at[q], info_send.at[0], info_recv.at[q], across(half - 1))

    def raw_copy(c):
        return remote(mine.at[c], raw.at[q, c], raw_send.at[c], raw_recv.at[q, c],
                      across(half - 1))

    def part_copy(j, c):
        return remote(part_out.at[j, c], part_in.at[c], part_send.at[j, c], part_recv.at[c],
                      across(j))

    def whole(ref, sem):
        return pltpu.make_async_copy(ref, ref, sem)

    def ship(b, g, c):
        for p in range(half):
            @pl.loop(0, n_seq)
            def _(r):
                @pl.when((r != 0) | (q != p))
                def _():
                    remote(packed.at[b, c, p * n_seq + r], received.at[g, c, r],
                           slot_send.at[b, c], slot_recv.at[g, c], near(r, p)).start()

        received[g, c, 0:1] = packed[b, c, pl.ds(q * n_seq, 1)]

    def seat_here(g):
        return jnp.minimum(g, half - 1) == q

    def fold(y, count):
        y = y.reshape(count, slots, wide)
        return jnp.concatenate([y[:, :, :fold_w], y[:, :, fold_w:]], axis=1).astype(BF16)

    def unfold(y, count):
        y = y.astype(F32)
        return (y[:, :slots].reshape(count * slots, fold_w).astype(BF16),
                y[:, slots:].reshape(count * slots, fold_w).astype(BF16))

    def pack(b, block, c):
        y = jnp.dot(pick[b], block, preferred_element_type=F32)
        packed[b, c] = fold(y, peers)

    square = lax.broadcasted_iota(jnp.int32, (n, n), 0)
    cross = lax.broadcasted_iota(jnp.int32, (n, n), 1)
    limit = jnp.sum(jnp.where(square == cross, capacity[...].astype(F32), 0.0),
                    axis=1, keepdims=True)
    expert = lax.broadcasted_iota(jnp.int32, (n, 1), 0).astype(F32)
    expert_seq = jnp.floor((expert + 0.5) / n_sub)
    expert_sub = (expert - expert_seq * n_sub).astype(jnp.int32)
    away = expert_seq.astype(jnp.int32) - s
    away = jnp.where(away < 0, away + n_seq, away)
    depth = jnp.where(side == 0, expert_sub, n_sub - 1 - expert_sub)
    seats = jnp.where(depth < half, (depth * n_seq + away) * slots, -1).astype(F32)

    def tables(ids, b):
        places = lax.broadcasted_iota(jnp.int32, (n, rows), 0)
        named = [(places == ids[k:k + 1, :]).astype(F32) for k in range(2)]
        before = (lax.broadcasted_iota(jnp.int32, (rows, rows), 0)
                  < lax.broadcasted_iota(jnp.int32, (rows, rows), 1))
        earlier = jnp.dot((named[0] + named[1]).astype(BF16), before.astype(F32).astype(BF16),
                          preferred_element_type=F32)
        slot, weight = [], []
        for k in range(2):
            rank = jnp.sum(named[k] * earlier, axis=0, keepdims=True)
            most = jnp.sum(named[k] * limit, axis=0, keepdims=True)
            seat = jnp.sum(named[k] * seats, axis=0, keepdims=True)
            kept = (rank < most) & (seat >= 0.0)
            slot.append(jnp.where(kept, seat + rank, -1.0).astype(jnp.int32))
            weight.append(ids[2 + k:3 + k, :].astype(F32) / 65536.0)
        at = lax.broadcasted_iota(jnp.int32, (peers * slots, rows), 0)
        first, second = at == slot[0], at == slot[1]
        pick[b] = (jnp.where(first, 1.0, 0.0) + jnp.where(second, 1.0, 0.0)).astype(BF16)
        full = jnp.where(first, weight[0], 0.0) + jnp.where(second, weight[1], 0.0)
        mix[b] = full.T.astype(BF16)

    tables(route[...], 0)

    fetch_tokens.wait()
    for c in range(CHUNKS):
        fetch_split(c).wait()
        for k in range(0, wide, TILE):
            mine[c, :, k:k + TILE] = jnp.dot(
                tokens[...], w_split[c, :, k:k + TILE], preferred_element_type=F32).astype(BF16)
        if c == 0:
            fetch_in.start()
            fetch_out.start()
            pl.semaphore_wait(barrier, peers - 1 + jnp.where(inner, half, 1))
            info_copy().start()

        @pl.when(~inner | (half == 1))
        def _():
            raw_copy(c).start()

        pack(0, mine[c], c)
        ship(0, q, c)

    fetch_merge.start()

    @pl.when(inner)
    def _():
        @pl.loop(0, half)
        def _(j):
            whole(info.at[j], info_recv.at[j]).wait()
            tables(info[j], 1 + j)

    def proxy(j, first, last):
        @pl.when(inner)
        def _():
            for c in range(first, last):
                whole(raw.at[j, c], raw_recv.at[j, c]).wait()
                pack(1 + j, raw[j, c], c)
                ship(1 + j, half + j, c)
                if j == 0 and half > 1:
                    for own in range(CHUNKS):
                        if min(own + LAG, CHUNKS - 1) == c:
                            raw_copy(own).start()

    def ffn(g):
        for c in range(CHUNKS):
            @pl.when(seat_here(g))
            def _():
                whole(received.at[g, c, pl.ds(0, n_seq - 1)], slot_recv.at[g, c]).wait()

            @pl.when(~seat_here(g))
            def _():
                whole(received.at[g, c], slot_recv.at[g, c]).wait()

            left, right = unfold(received[g, c], n_seq)
            x[:, c * wide:c * wide + fold_w] = left
            x[:, c * wide + fold_w:(c + 1) * wide] = right

        @pl.loop(0, ffe // TILE)
        def _(t):
            gate_at = pl.ds(pl.multiple_of(t * TILE, TILE), TILE)
            up_at = pl.ds(pl.multiple_of(ffe + t * TILE, TILE), TILE)
            gate = jnp.dot(x[...], w_in[:, gate_at], preferred_element_type=F32)
            up = jnp.dot(x[...], w_in[:, up_at], preferred_element_type=F32)
            hidden[:, gate_at] = (gate / (1.0 + jnp.exp(-gate)) * up).astype(BF16)

        to = jnp.minimum(g, half - 1)
        b = jnp.maximum(g - half + 1, 0)
        for c in range(CHUNKS):
            y = jnp.dot(hidden[...], w_out[:, c * wide:(c + 1) * wide],
                        preferred_element_type=F32)
            answers[g, c] = fold(y, n_seq)

            @pl.loop(0, n_seq)
            def _(r):
                @pl.when((r != 0) | (q != to))
                def _():
                    remote(answers.at[g, c, r], returned.at[b, c, q * n_seq + r],
                           ans_send.at[g, c], ans_recv.at[b, c],
                           near(n_seq - r, to)).start()

            @pl.when(q == to)
            def _():
                returned[b, c, pl.ds(q * n_seq, 1)] = answers[g, c, 0:1]

    def combine(b, c):
        whole(returned.at[b, c, pl.ds(0, peers - 1)], ans_recv.at[b, c]).wait()
        left, right = unfold(returned[b, c], peers)
        return jnp.dot(mix[b], jnp.concatenate([left, right], axis=1),
                       preferred_element_type=F32)

    def bring_back(j):
        @pl.when(inner)
        def _():
            for c in range(CHUNKS):
                part_out[j, c] = combine(1 + j, c).astype(BF16)
                part_copy(j, c).start()

    fetch_in.wait()
    fetch_out.wait()
    middle = CHUNKS // 2
    proxy(0, 0, middle)
    ffn(q)
    proxy(0, middle, CHUNKS)
    for i in range(1, half):
        ffn(lax.rem(q + i, half))
    for j in range(half):
        last = j == half - 1
        if j > 0:
            proxy(j, 0, CHUNKS)
        if last:
            for c in range(CHUNKS):
                acc[:, c * wide:(c + 1) * wide] = combine(0, c)
            for k in range(half - 1):
                bring_back(k)
        ffn(half + j)
    bring_back(half - 1)

    for c in range(CHUNKS):
        at = slice(c * wide, (c + 1) * wide)
        whole(part_in.at[c], part_recv.at[c]).wait()
        head[:, at] = (acc[:, at] + part_in[c].astype(F32)).astype(BF16)

    fetch_merge.wait()
    tiles = width // TILE

    def target(j):
        low = jnp.where(j < n_sub - 1 - z, n_sub - 1 - j, j - (n_sub - 1 - z))
        high = jnp.where(j < z, j, n_sub - 1 - (j - z))
        return jnp.where(z < n_sub // 2, low, high)

    def share(t, k):
        cols = pl.ds(pl.multiple_of(t * width + k * TILE, TILE), TILE)
        return jnp.dot(head[...], w_merge[:, cols], preferred_element_type=F32)

    def hop(t, k):
        up = t > z
        to = jnp.where(up, z + 1, z - 1)
        place = jnp.where(up | (t != z - 1), t, n_sub)
        return remote(sending.at[t, k], landed.at[place, k], hop_send.at[t, k],
                      hop_recv.at[place, k], (s, to))

    for j in range(n_sub - 1):
        t = target(j)
        edge = jnp.where(t > z, z == 0, z == n_sub - 1)

        @pl.loop(0, tiles)
        def _(k):
            total = share(t, k)

            @pl.when(edge)
            def _():
                sending[t, k] = total.astype(BF16)

            @pl.when(~edge)
            def _():
                whole(landed.at[t, k], hop_recv.at[t, k]).wait()
                sending[t, k] = (total + landed[t, k].astype(F32)).astype(BF16)

            hop(t, k).start()

    for k in range(tiles):
        acc[:, k * TILE:(k + 1) * TILE] = share(z, k)
    for place, has in ((z, z > 0), (n_sub, z < n_sub - 1)):
        @pl.when(has)
        def _():
            for k in range(tiles):
                whole(landed.at[place, k], hop_recv.at[place, k]).wait()
                acc[:, k * TILE:(k + 1) * TILE] += landed[place, k].astype(F32)

    out[...] = acc[...].astype(out.dtype)

    whole(route, info_send.at[0]).wait()
    for c in range(CHUNKS):
        whole(mine.at[c], raw_send.at[c]).wait()
        whole(packed.at[0, c, pl.ds(0, peers - 1)], slot_send.at[0, c]).wait()
        for g in range(n_sub):
            @pl.when(seat_here(g))
            def _():
                whole(answers.at[g, c, pl.ds(0, n_seq - 1)], ans_send.at[g, c]).wait()

            @pl.when(~seat_here(g))
            def _():
                whole(answers.at[g, c], ans_send.at[g, c]).wait()

        @pl.when(inner)
        def _():
            for j in range(half):
                whole(packed.at[1 + j, c, pl.ds(0, peers - 1)], slot_send.at[1 + j, c]).wait()
                whole(part_out.at[j, c], part_send.at[j, c]).wait()

    for t in range(n_sub):
        @pl.when(z != t)
        def _():
            for k in range(tiles):
                whole(sending.at[t, k], hop_send.at[t, k]).wait()


def layer(n_seq, n_sub, slots, route, capacity, tokens, w_split, w_in, w_out, w_merge):
    half = n_sub // 2
    rows, width = tokens.shape[0], w_out.shape[1]
    peers, wide, tiles = half * n_seq, width // CHUNKS, width // TILE
    vmem = pl.BlockSpec(memory_space=pltpu.VMEM)
    hbm = pl.BlockSpec(memory_space=pltpu.HBM)

    def buf(*shape, dtype=BF16):
        return pltpu.VMEM(shape, dtype)

    dma = pltpu.SemaphoreType.DMA
    message = (2 * slots, wide // 2)
    return pl.pallas_call(
        functools.partial(layer_kernel, n_seq, n_sub, slots),
        out_shape=jax.ShapeDtypeStruct((rows, width), BF16),
        in_specs=[vmem] * 2 + [hbm] * 5,
        out_specs=vmem,
        scratch_shapes=[
            buf(*tokens.shape),
            buf(CHUNKS, w_split.shape[0], wide),
            buf(*w_in.shape),
            buf(*w_out.shape),
            buf(*w_merge.shape),
            buf(half, *route.shape, dtype=jnp.int32),
            buf(CHUNKS, rows, wide),
            buf(half, CHUNKS, rows, wide),
            buf(1 + half, peers * slots, rows),
            buf(1 + half, rows, peers * slots),
            buf(1 + half, CHUNKS, peers, *message),
            buf(n_sub, CHUNKS, n_seq, *message),
            buf(n_seq * slots, width),
            buf(n_seq * slots, w_out.shape[0]),
            buf(n_sub, CHUNKS, n_seq, *message),
            buf(1 + half, CHUNKS, peers, *message),
            buf(half, CHUNKS, rows, wide),
            buf(CHUNKS, rows, wide),
            buf(rows, width, dtype=F32),
            buf(rows, width),
            buf(n_sub, tiles, rows, TILE),
            buf(n_sub + 1, tiles, rows, TILE),
            dma((CHUNKS + 4,)),
            dma((1,)),
            dma((half,)),
            dma((CHUNKS,)),
            dma((half, CHUNKS)),
            dma((1 + half, CHUNKS)),
            dma((n_sub, CHUNKS)),
            dma((n_sub, CHUNKS)),
            dma((1 + half, CHUNKS)),
            dma((half, CHUNKS)),
            dma((CHUNKS,)),
            dma((n_sub, tiles)),
            dma((n_sub + 1, tiles)),
        ],
        compiler_params=pltpu.CompilerParams(
            collective_id=1, has_side_effects=True, vmem_limit_bytes=VMEM_BYTES),
        name="layer",
    )(route, capacity, tokens, w_split, w_in, w_out, w_merge)


def body(n_seq, n_sub, tokens, w_split, w_merge, expert_in, expert_out, expert_ids, combine_q,
         capacity):
    experts = capacity.shape[0]
    slot_count = -(-(3 * tokens.shape[0] // experts) // 8) * 8
    route = jnp.concatenate([expert_ids[0].T, combine_q[0].T], axis=0)
    return layer(n_seq, n_sub, slot_count, route, capacity[None, :], tokens, w_split,
                 expert_in[0], expert_out[0], w_merge)


def solution(mesh):
    in_specs = (
        P("seq", None),
        P(None, "sub"),
        P("sub", None),
        P(("seq", "sub"), None, None),
        P(("seq", "sub"), None, None),
        P("sub", "seq", None),
        P("sub", "seq", None),
        P(),
    )
    out_specs = P("seq", "sub")
    call = functools.partial(body, mesh.shape["seq"], mesh.shape["sub"])
    return jax.shard_map(call, mesh=mesh, in_specs=in_specs, out_specs=out_specs, check_vma=False)
```

```python
import functools

import jax
import jax.numpy as jnp
from jax import lax
from jax.experimental import pallas as pl
from jax.experimental.pallas import tpu as pltpu
from jax.sharding import PartitionSpec as P

MESH = pl.DeviceIdType.MESH
scope = jax.named_scope
TILE = 256
CHUNKS = 2
PARTS = 2 * CHUNKS
EARLY = 1
VMEM_BYTES = 60 * 1024 * 1024
F32 = jnp.float32
BF16 = jnp.bfloat16


def layer_kernel(n_seq, n_sub, slots, route, capacity, tokens_hbm, w_split_hbm, w_in_hbm,
                 w_out_hbm, w_merge_hbm, out,
                 tokens, w_split, w_in, w_out, w_merge, info, mine, raw, pick, mix, packed,
                 received, x, hidden, answers, returned, part_out, part_in, acc, head,
                 sending, landed,
                 load_sem, info_send, info_recv, raw_send, raw_recv, slot_send, slot_recv,
                 ans_send, ans_recv, back_send, back_recv, part_send, part_recv,
                 hop_send, hop_recv):
    s, z = lax.axis_index("seq"), lax.axis_index("sub")
    half = n_sub // 2
    last = half - 1
    side = z // half
    q = jnp.where(side == 0, z, n_sub - 1 - z)
    inner = q == last
    n = n_seq * n_sub
    peers = half * n_seq
    rows, width = acc.shape
    part = width // PARTS
    ffe = w_out.shape[0]
    group = n_seq * slots
    outers = range(last)

    def plane(where, depth):
        return jnp.where(where == 0, depth, n_sub - 1 - depth)

    def near(r, depth):
        return (lax.rem(s + r, n_seq), plane(side, depth))

    def across():
        return (s, plane(1 - side, last))

    fetch_tokens = pltpu.make_async_copy(tokens_hbm, tokens, load_sem.at[PARTS])
    fetch_in = pltpu.make_async_copy(w_in_hbm, w_in, load_sem.at[PARTS + 1])
    fetch_out = pltpu.make_async_copy(w_out_hbm, w_out, load_sem.at[PARTS + 2])
    fetch_merge = pltpu.make_async_copy(w_merge_hbm, w_merge, load_sem.at[PARTS + 3])

    def fetch_split(i):
        return pltpu.make_async_copy(
            w_split_hbm.at[:, pl.ds(i * part, part)], w_split.at[i], load_sem.at[i])

    fetch_tokens.start()
    fetch_split(0).start()

    barrier = pltpu.get_barrier_semaphore()
    for p in range(half):
        @pl.loop(0, n_seq)
        def _(r):
            @pl.when((r != 0) | (q != p))
            def _():
                pl.semaphore_signal(barrier, inc=1, device_id=near(r, p), device_id_type=MESH)

        @pl.when(inner | (p == last))
        def _():
            pl.semaphore_signal(barrier, inc=1, device_id=(s, plane(1 - side, p)),
                                device_id_type=MESH)

    def remote(src, dst, send, recv, to):
        return pltpu.make_async_remote_copy(src_ref=src, dst_ref=dst, send_sem=send,
                                            recv_sem=recv, device_id=to, device_id_type=MESH)

    def whole(ref, sem):
        return pltpu.make_async_copy(ref, ref, sem)

    def info_near():
        return remote(route, info.at[q], info_send.at[0], info_recv.at[q], (s, plane(side, last)))

    def info_across():
        return remote(route, info.at[half + q], info_send.at[1], info_recv.at[half + q], across())

    def raw_across(i):
        return remote(mine.at[i], raw.at[q, i], raw_send.at[i], raw_recv.at[q, i], across())

    def part_across(g, i):
        return remote(part_out.at[half + g, i], part_in.at[g, i], part_send.at[half + g, i],
                      part_recv.at[g, i], across())

    def part_outward(g, i):
        return remote(part_out.at[g, i], part_in.at[g, i], part_send.at[g, i],
                      part_recv.at[g, i], (s, plane(side, g)))

    def ship(g, c, p):
        with scope("ship"):
            @pl.loop(0, n_seq)
            def _(r):
                @pl.when((r != 0) | (q != p))
                def _():
                    remote(packed.at[g, c, p, r], received.at[g, c, r], slot_send.at[g, c, p],
                           slot_recv.at[g, c], near(r, p)).start()

            @pl.when(q == p)
            def _():
                received[g, c, 0:1] = packed[g, c, p, 0:1]

    def unfold(y):
        y = y.astype(F32)
        return (y[:, :slots].reshape(group, part).astype(BF16),
                y[:, slots:].reshape(group, part).astype(BF16))

    def pack(g, p, block, c):
        with scope("pack"):
            y = [jnp.dot(pick[g, p], block(2 * c + k), preferred_element_type=F32)
                 .reshape(n_seq, slots, part) for k in range(2)]
            packed[g, c, p] = jnp.concatenate(y, axis=1).astype(BF16)

    square = lax.broadcasted_iota(jnp.int32, (n, n), 0)
    cross = lax.broadcasted_iota(jnp.int32, (n, n), 1)
    limit = jnp.sum(jnp.where(square == cross, capacity[...].astype(F32), 0.0),
                    axis=1, keepdims=True)
    expert = lax.broadcasted_iota(jnp.int32, (n, 1), 0).astype(F32)
    expert_seq = jnp.floor((expert + 0.5) / n_sub)
    expert_sub = (expert - expert_seq * n_sub).astype(jnp.int32)
    away = expert_seq.astype(jnp.int32) - s
    away = jnp.where(away < 0, away + n_seq, away)
    depth = jnp.where(side == 0, expert_sub, n_sub - 1 - expert_sub)
    seats = jnp.where(depth < half, (depth * n_seq + away) * slots, -1).astype(F32)

    def tables(ids, g, wanted):
        places = lax.broadcasted_iota(jnp.int32, (n, rows), 0)
        named = [(places == ids[k:k + 1, :]).astype(F32) for k in range(2)]
        before = (lax.broadcasted_iota(jnp.int32, (rows, rows), 0)
                  < lax.broadcasted_iota(jnp.int32, (rows, rows), 1))
        earlier = jnp.dot((named[0] + named[1]).astype(BF16), before.astype(F32).astype(BF16),
                          preferred_element_type=F32)
        slot, weight = [], []
        for k in range(2):
            rank = jnp.sum(named[k] * earlier, axis=0, keepdims=True)
            most = jnp.sum(named[k] * limit, axis=0, keepdims=True)
            seat = jnp.sum(named[k] * seats, axis=0, keepdims=True)
            kept = (rank < most) & (seat >= 0.0)
            slot.append(jnp.where(kept, seat + rank, -1.0).astype(jnp.int32))
            weight.append(ids[2 + k:3 + k, :].astype(F32) / 65536.0)
        for p in range(half):
            if wanted(p):
                at = lax.broadcasted_iota(jnp.int32, (group, rows), 0) + p * group
                first, second = at == slot[0], at == slot[1]
                pick[g, p] = (jnp.where(first, 1.0, 0.0) + jnp.where(second, 1.0, 0.0)).astype(BF16)
                full = jnp.where(first, weight[0], 0.0) + jnp.where(second, weight[1], 0.0)
                mix[g, p] = full.T.astype(BF16)

    with scope("tables"):
        tables(route[...], q, lambda p: True)

    with scope("w_tokens"):
        fetch_tokens.wait()
    for i in range(1, PARTS):
        fetch_split(i).start()
    fetch_in.start()
    fetch_out.start()

    def pack_own(c):
        for p in range(half):
            pack(q, p, lambda i: mine[i], c)

            @pl.when(inner | (q == p))
            def _():
                ship(q, c, p)

    for i in range(PARTS):
        with scope("w_split"):
            fetch_split(i).wait()
        with scope("split"):
            mine[i] = jnp.dot(tokens[...], w_split[i], preferred_element_type=F32).astype(BF16)
        if i == 0:
            with scope("w_barrier"):
                pl.semaphore_wait(barrier, peers - 1 + jnp.where(inner, half, 1))
            info_across().start()

            @pl.when(~inner)
            def _():
                info_near().start()

        @pl.when(~inner | (half == 1) | (i < EARLY))
        def _():
            raw_across(i).start()

        if i % 2 == 1:
            @pl.when(inner)
            def _():
                pack_own(i // 2)

    fetch_merge.start()

    def proxy(g, c):
        for i in (2 * c, 2 * c + 1):
            with scope(f"w_raw{g}"):
                whole(raw.at[g - half, i], raw_recv.at[g - half, i]).wait()
        for p in range(half):
            pack(g, p, lambda i: raw[g - half, i], c)
            ship(g, c, p)

    def ffn(k, g):
        for c in range(CHUNKS):
            with scope(f"w_slots{k}"):
                direct = q != jnp.minimum(g, last)

                @pl.when(direct)
                def _():
                    whole(received.at[g, c], slot_recv.at[g, c]).wait()

                @pl.when(jnp.logical_not(direct))
                def _():
                    whole(received.at[g, c, pl.ds(0, n_seq - 1)], slot_recv.at[g, c]).wait()
            with scope("unfold"):
                left, right = unfold(received[g, c])
                x[:, 2 * c * part:(2 * c + 1) * part] = left
                x[:, (2 * c + 1) * part:(2 * c + 2) * part] = right

        with scope("gate_up"):
            @pl.loop(0, ffe // TILE)
            def _(t):
                gate_at = pl.ds(pl.multiple_of(t * TILE, TILE), TILE)
                up_at = pl.ds(pl.multiple_of(ffe + t * TILE, TILE), TILE)
                gate = jnp.dot(x[...], w_in[:, gate_at], preferred_element_type=F32)
                up = jnp.dot(x[...], w_in[:, up_at], preferred_element_type=F32)
                hidden[:, gate_at] = (gate / (1.0 + jnp.exp(-gate)) * up).astype(BF16)

        for c in range(CHUNKS):
            with scope("down"):
                y = [jnp.dot(hidden[...], w_out[:, i * part:(i + 1) * part],
                             preferred_element_type=F32).reshape(n_seq, slots, part)
                     for i in (2 * c, 2 * c + 1)]
                answers[g, c] = jnp.concatenate(y, axis=1).astype(BF16)

    def reply(g):
        for c in range(CHUNKS):
            with scope("reply"):
                @pl.loop(1, n_seq)
                def _(r):
                    remote(answers.at[g, c, r], returned.at[g, c, q * n_seq + r],
                           ans_send.at[g, c], ans_recv.at[g, c], near(n_seq - r, q)).start()

                returned[g, c, pl.ds(q * n_seq, 1)] = answers[g, c, 0:1]

    def mine_at(g, c, p):
        return returned.at[g, c, pl.ds(p * n_seq, n_seq)]

    def gathered(g, c):
        with scope("w_gather"):
            whole(returned.at[g, c, pl.ds(0, n_seq - 1)], ans_recv.at[g, c]).wait()

    def inward(g, c):
        return remote(mine_at(g, c, q), mine_at(g, c, q), back_send.at[g, c],
                      back_recv.at[g, c, q], (s, plane(side, last)))

    def pass_inward(g):
        for c in range(CHUNKS):
            gathered(g, c)
            inward(g, c).start()

    def combine(g, c, planes, tag):
        gathered(g, c)
        with scope(f"w_reply{tag}"):
            for p in planes:
                if p != last:
                    whole(mine_at(g, c, p), back_recv.at[g, c, p]).wait()
        with scope("combine"):
            total = [None, None]
            for p in planes:
                halves = unfold(returned[g, c, pl.ds(p * n_seq, n_seq)])
                for k in range(2):
                    y = jnp.dot(mix[g, p], halves[k], preferred_element_type=F32)
                    total[k] = y if total[k] is None else total[k] + y
            return total

    every = list(range(half))

    def bring_across(g):
        for c in range(CHUNKS):
            sums = combine(half + g, c, every, half + g)
            for k in range(2):
                part_out[half + g, 2 * c + k] = sums[k].astype(BF16)
                part_across(g, 2 * c + k).start()

    def bring_outward(g):
        for c in range(CHUNKS):
            sums = combine(g, c, [p for p in every if p != g], g)
            for k in range(2):
                i = 2 * c + k
                with scope("w_part"):
                    whole(part_in.at[g, i], part_recv.at[g, i]).wait()
                part_out[g, i] = (sums[k] + part_in[g, i].astype(F32)).astype(BF16)
                part_outward(g, i).start()

    def learn(g):
        with scope("w_info"):
            whole(info.at[g], info_recv.at[g]).wait()
        with scope("tables"):
            tables(info[g], g, lambda p: p != g)

    with scope("w_load"):
        fetch_in.wait()
        fetch_out.wait()

    @pl.when(inner)
    def _():
        learn(half)
        proxy(half, 0)
        ffn(0, last)
        for c in range(1, CHUNKS):
            proxy(half, c)
        if half > 1:
            for i in range(EARLY, PARTS):
                raw_across(i).start()
        for g in [*range(half + 1, n_sub), *outers]:
            learn(g)
        for g in range(half + 1, n_sub):
            proxy(g, 0)
            ffn(g - 1, g - 1)
            for c in range(1, CHUNKS):
                proxy(g, c)
            reply(g - 1)
        for g in outers:
            ffn(1 + g, g)
        ffn(n_sub - 1, n_sub - 1)
        for g in outers:
            reply(g)
        reply(n_sub - 1)
        reply(last)
        for g in outers:
            bring_across(g)
        for g in outers:
            bring_outward(g)
        bring_across(last)
        for c in range(CHUNKS):
            sums = combine(last, c, every, "own")
            for k in range(2):
                i = 2 * c + k
                acc[:, i * part:(i + 1) * part] = sums[k]

    @pl.when(~inner)
    def _():
        for c in range(CHUNKS):
            pack_own(c)
        with scope("w_sent"):
            for i in range(PARTS):
                whole(mine.at[i], raw_send.at[i]).wait()
        for c in range(CHUNKS):
            for p in range(half):
                @pl.when(q != p)
                def _():
                    ship(q, c, p)

        ffn(1, last)
        reply(last)
        ffn(0, q)
        pass_inward(last)
        for g in range(half, n_sub):
            ffn(g, g)
            reply(g)
            pass_inward(g)
            if g == half:
                reply(q)

        for g in outers:
            @pl.when(q != g)
            def _():
                ffn(n_sub, g)
                reply(g)
                pass_inward(g)

    for g in outers:
        @pl.when(q == g)
        def _():
            for c in range(CHUNKS):
                gathered(g, c)
                halves = unfold(returned[g, c, pl.ds(g * n_seq, n_seq)])
                for k in range(2):
                    i = 2 * c + k
                    acc[:, i * part:(i + 1) * part] = jnp.dot(
                        mix[g, g], halves[k], preferred_element_type=F32)

    for i in range(PARTS):
        at = slice(i * part, (i + 1) * part)
        with scope("w_part"):
            whole(part_in.at[q, i], part_recv.at[q, i]).wait()
        head[:, at] = (acc[:, at] + part_in[q, i].astype(F32)).astype(BF16)

    with scope("w_merge"):
        fetch_merge.wait()
    tiles = width // TILE

    def target(j):
        low = jnp.where(j < n_sub - 1 - z, n_sub - 1 - j, j - (n_sub - 1 - z))
        high = jnp.where(j < z, j, n_sub - 1 - (j - z))
        return jnp.where(z < n_sub // 2, low, high)

    def share(t, k):
        cols = pl.ds(pl.multiple_of(t * width + k * TILE, TILE), TILE)
        return jnp.dot(head[...], w_merge[:, cols], preferred_element_type=F32)

    def hop(t, k):
        up = t > z
        to = jnp.where(up, z + 1, z - 1)
        place = jnp.where(up | (t != z - 1), t, n_sub)
        return remote(sending.at[t, k], landed.at[place, k], hop_send.at[t, k],
                      hop_recv.at[place, k], (s, to))

    for j in range(n_sub - 1):
        t = target(j)
        edge = jnp.where(t > z, z == 0, z == n_sub - 1)

        with scope(f"merge{j}"):
            @pl.loop(0, tiles)
            def _(k):
                total = share(t, k)

                @pl.when(edge)
                def _():
                    sending[t, k] = total.astype(BF16)

                @pl.when(~edge)
                def _():
                    whole(landed.at[t, k], hop_recv.at[t, k]).wait()
                    sending[t, k] = (total + landed[t, k].astype(F32)).astype(BF16)

                hop(t, k).start()

    with scope("merge_own"):
        for k in range(tiles):
            acc[:, k * TILE:(k + 1) * TILE] = share(z, k)
    for place, has in ((z, z > 0), (n_sub, z < n_sub - 1)):
        with scope("w_landed"):
            @pl.when(has)
            def _():
                for k in range(tiles):
                    whole(landed.at[place, k], hop_recv.at[place, k]).wait()
                    acc[:, k * TILE:(k + 1) * TILE] += landed[place, k].astype(F32)

    with scope("finish"):
        out[...] = acc[...].astype(out.dtype)

    whole(route, info_send.at[1]).wait()

    @pl.when(~inner)
    def _():
        whole(route, info_send.at[0]).wait()

    @pl.when(inner)
    def _():
        for i in range(PARTS):
            whole(mine.at[i], raw_send.at[i]).wait()

    for g in range(n_sub):
        sender = (q == g) | (inner & (g >= half))
        for c in range(CHUNKS):
            whole(answers.at[g, c, pl.ds(0, n_seq - 1)], ans_send.at[g, c]).wait()

            @pl.when(~inner & (q != g))
            def _():
                whole(mine_at(g, c, q), back_send.at[g, c]).wait()

            for p in range(half):
                @pl.when(sender & (q == p))
                def _():
                    whole(received.at[g, c, pl.ds(0, n_seq - 1)], slot_send.at[g, c, p]).wait()

                @pl.when(sender & (q != p))
                def _():
                    whole(received.at[g, c], slot_send.at[g, c, p]).wait()

    @pl.when(inner)
    def _():
        for g in range(n_sub):
            for i in range(PARTS):
                if g != last:
                    whole(part_out.at[g, i], part_send.at[g, i]).wait()

    for t in range(n_sub):
        @pl.when(z != t)
        def _():
            for k in range(tiles):
                whole(sending.at[t, k], hop_send.at[t, k]).wait()


def layer(n_seq, n_sub, slots, route, capacity, tokens, w_split, w_in, w_out, w_merge):
    half = n_sub // 2
    rows, width = tokens.shape[0], w_out.shape[1]
    peers, part, tiles = half * n_seq, width // PARTS, width // TILE
    vmem = pl.BlockSpec(memory_space=pltpu.VMEM)
    hbm = pl.BlockSpec(memory_space=pltpu.HBM)

    def buf(*shape, dtype=BF16):
        return pltpu.VMEM(shape, dtype)

    dma = pltpu.SemaphoreType.DMA
    message = (2 * slots, part)
    group = n_seq * slots
    return pl.pallas_call(
        functools.partial(layer_kernel, n_seq, n_sub, slots),
        out_shape=jax.ShapeDtypeStruct((rows, width), BF16),
        in_specs=[vmem] * 2 + [hbm] * 5,
        out_specs=vmem,
        scratch_shapes=[
            buf(*tokens.shape),
            buf(PARTS, w_split.shape[0], part),
            buf(*w_in.shape),
            buf(*w_out.shape),
            buf(*w_merge.shape),
            buf(n_sub, *route.shape, dtype=jnp.int32),
            buf(PARTS, rows, part),
            buf(half, PARTS, rows, part),
            buf(n_sub, half, group, rows),
            buf(n_sub, half, rows, group),
            buf(n_sub, CHUNKS, half, n_seq, *message),
            buf(n_sub, CHUNKS, n_seq, *message),
            buf(group, width),
            buf(group, w_out.shape[0]),
            buf(n_sub, CHUNKS, n_seq, *message),
            buf(n_sub, CHUNKS, peers, *message),
            buf(n_sub, PARTS, rows, part),
            buf(half, PARTS, rows, part),
            buf(rows, width, dtype=F32),
            buf(rows, width),
            buf(n_sub, tiles, rows, TILE),
            buf(n_sub + 1, tiles, rows, TILE),
            dma((PARTS + 4,)),
            dma((2,)),
            dma((n_sub,)),
            dma((PARTS,)),
            dma((half, PARTS)),
            dma((n_sub, CHUNKS, half)),
            dma((n_sub, CHUNKS)),
            dma((n_sub, CHUNKS)),
            dma((n_sub, CHUNKS)),
            dma((n_sub, CHUNKS)),
            dma((n_sub, CHUNKS, half)),
            dma((n_sub, PARTS)),
            dma((half, PARTS)),
            dma((n_sub, tiles)),
            dma((n_sub + 1, tiles)),
        ],
        compiler_params=pltpu.CompilerParams(
            collective_id=1, has_side_effects=True, vmem_limit_bytes=VMEM_BYTES),
        name="layer",
    )(route, capacity, tokens, w_split, w_in, w_out, w_merge)


def body(n_seq, n_sub, tokens, w_split, w_merge, expert_in, expert_out, expert_ids, combine_q,
         capacity):
    experts = capacity.shape[0]
    slot_count = -(-(3 * tokens.shape[0] // experts) // 8) * 8
    route = jnp.concatenate([expert_ids[0].T, combine_q[0].T], axis=0)
    return layer(n_seq, n_sub, slot_count, route, capacity[None, :], tokens, w_split,
                 expert_in[0], expert_out[0], w_merge)


def solution(mesh):
    in_specs = (
        P("seq", None),
        P(None, "sub"),
        P("sub", None),
        P(("seq", "sub"), None, None),
        P(("seq", "sub"), None, None),
        P("sub", "seq", None),
        P("sub", "seq", None),
        P(),
    )
    out_specs = P("seq", "sub")
    call = functools.partial(body, mesh.shape["seq"], mesh.shape["sub"])
    return jax.shard_map(call, mesh=mesh, in_specs=in_specs, out_specs=out_specs, check_vma=False)
```

```python
import functools

import jax
import jax.numpy as jnp
from jax import lax
from jax.experimental import pallas as pl
from jax.experimental.pallas import tpu as pltpu
from jax.sharding import PartitionSpec as P

MESH = pl.DeviceIdType.MESH
scope = jax.named_scope
TILE = 256
CHUNKS = 2
PARTS = 2 * CHUNKS
EARLY = 1
VMEM_BYTES = 60 * 1024 * 1024
F32 = jnp.float32
BF16 = jnp.bfloat16


def layer_kernel(n_seq, n_sub, slots, ids_hbm, quanta_hbm, capacity, tokens_hbm, w_split_hbm, w_in_hbm,
                 w_out_hbm, w_merge_hbm, out,
                 tokens, w_split, w_in, w_out, w_merge, route, info, mine, raw, pick, mix, packed,
                 received, x, hidden, answers, returned, part_out, part_in, acc, head,
                 sending, landed,
                 load_sem, info_send, info_recv, raw_send, raw_recv, slot_send, slot_recv,
                 ans_send, ans_recv, back_send, back_recv, part_send, part_recv,
                 hop_send, hop_recv):
    s, z = lax.axis_index("seq"), lax.axis_index("sub")
    half = n_sub // 2
    last = half - 1
    side = z // half
    q = jnp.where(side == 0, z, n_sub - 1 - z)
    inner = q == last
    n = n_seq * n_sub
    peers = half * n_seq
    rows, width = acc.shape
    part = width // PARTS
    ffe = w_out.shape[0]
    group = n_seq * slots
    outers = range(last)

    def plane(where, depth):
        return jnp.where(where == 0, depth, n_sub - 1 - depth)

    def near(r, depth):
        return (lax.rem(s + r, n_seq), plane(side, depth))

    def across():
        return (s, plane(1 - side, last))

    fetch_tokens = pltpu.make_async_copy(tokens_hbm, tokens, load_sem.at[PARTS])
    fetch_in = pltpu.make_async_copy(w_in_hbm, w_in, load_sem.at[PARTS + 1])
    fetch_out = pltpu.make_async_copy(w_out_hbm, w_out, load_sem.at[PARTS + 2])
    fetch_merge = pltpu.make_async_copy(w_merge_hbm, w_merge, load_sem.at[PARTS + 3])

    def fetch_split(i):
        return pltpu.make_async_copy(
            w_split_hbm.at[:, pl.ds(i * part, part)], w_split.at[i], load_sem.at[i])

    fetch_ids = pltpu.make_async_copy(ids_hbm, route.at[0], load_sem.at[PARTS + 4])
    fetch_quanta = pltpu.make_async_copy(quanta_hbm, route.at[1], load_sem.at[PARTS + 5])
    fetch_ids.start()
    fetch_quanta.start()
    fetch_tokens.start()
    fetch_split(0).start()

    barrier = pltpu.get_barrier_semaphore()
    for p in range(half):
        @pl.loop(0, n_seq)
        def _(r):
            @pl.when((r != 0) | (q != p))
            def _():
                pl.semaphore_signal(barrier, inc=1, device_id=near(r, p), device_id_type=MESH)

        @pl.when(inner | (p == last))
        def _():
            pl.semaphore_signal(barrier, inc=1, device_id=(s, plane(1 - side, p)),
                                device_id_type=MESH)

    def remote(src, dst, send, recv, to):
        return pltpu.make_async_remote_copy(src_ref=src, dst_ref=dst, send_sem=send,
                                            recv_sem=recv, device_id=to, device_id_type=MESH)

    def whole(ref, sem):
        return pltpu.make_async_copy(ref, ref, sem)

    def info_near():
        return remote(route, info.at[q], info_send.at[0], info_recv.at[q], (s, plane(side, last)))

    def info_across():
        return remote(route, info.at[half + q], info_send.at[1], info_recv.at[half + q], across())

    def raw_across(i):
        return remote(mine.at[i], raw.at[q, i], raw_send.at[i], raw_recv.at[q, i], across())

    def part_across(g, i):
        return remote(part_out.at[half + g, i], part_in.at[g, i], part_send.at[half + g, i],
                      part_recv.at[g, i], across())

    def part_outward(g, i):
        return remote(part_out.at[g, i], part_in.at[g, i], part_send.at[g, i],
                      part_recv.at[g, i], (s, plane(side, g)))

    def ship(g, c, p):
        with scope("ship"):
            @pl.loop(0, n_seq)
            def _(r):
                @pl.when((r != 0) | (q != p))
                def _():
                    remote(packed.at[g, c, p, r], received.at[g, c, r], slot_send.at[g, c, p],
                           slot_recv.at[g, c], near(r, p)).start()

            @pl.when(q == p)
            def _():
                received[g, c, 0:1] = packed[g, c, p, 0:1]

    def unfold(y):
        y = y.astype(F32)
        return (y[:, :slots].reshape(group, part).astype(BF16),
                y[:, slots:].reshape(group, part).astype(BF16))

    def pack(g, p, block, c):
        with scope("pack"):
            y = [jnp.dot(pick[g, p], block(2 * c + k), preferred_element_type=F32)
                 .reshape(n_seq, slots, part) for k in range(2)]
            packed[g, c, p] = jnp.concatenate(y, axis=1).astype(BF16)

    square = lax.broadcasted_iota(jnp.int32, (n, n), 0)
    cross = lax.broadcasted_iota(jnp.int32, (n, n), 1)
    limit = jnp.sum(jnp.where(square == cross, capacity[...].astype(F32), 0.0),
                    axis=1, keepdims=True)
    expert = lax.broadcasted_iota(jnp.int32, (n, 1), 0).astype(F32)
    expert_seq = jnp.floor((expert + 0.5) / n_sub)
    expert_sub = (expert - expert_seq * n_sub).astype(jnp.int32)
    away = expert_seq.astype(jnp.int32) - s
    away = jnp.where(away < 0, away + n_seq, away)
    depth = jnp.where(side == 0, expert_sub, n_sub - 1 - expert_sub)
    seats = jnp.where(depth < half, (depth * n_seq + away) * slots, -1).astype(F32)

    def tables(ids, g, wanted):
        places = lax.broadcasted_iota(jnp.int32, (n, rows), 0)
        named = [(places == ids[0, k:k + 1, :]).astype(F32) for k in range(2)]
        before = (lax.broadcasted_iota(jnp.int32, (rows, rows), 0)
                  < lax.broadcasted_iota(jnp.int32, (rows, rows), 1))
        earlier = jnp.dot((named[0] + named[1]).astype(BF16), before.astype(F32).astype(BF16),
                          preferred_element_type=F32)
        slot, weight = [], []
        for k in range(2):
            rank = jnp.sum(named[k] * earlier, axis=0, keepdims=True)
            most = jnp.sum(named[k] * limit, axis=0, keepdims=True)
            seat = jnp.sum(named[k] * seats, axis=0, keepdims=True)
            kept = (rank < most) & (seat >= 0.0)
            slot.append(jnp.where(kept, seat + rank, -1.0).astype(jnp.int32))
            weight.append(ids[1, k:k + 1, :].astype(F32) / 65536.0)
        for p in range(half):
            if wanted(p):
                at = lax.broadcasted_iota(jnp.int32, (group, rows), 0) + p * group
                first, second = at == slot[0], at == slot[1]
                pick[g, p] = (jnp.where(first, 1.0, 0.0) + jnp.where(second, 1.0, 0.0)).astype(BF16)
                full = jnp.where(first, weight[0], 0.0) + jnp.where(second, weight[1], 0.0)
                mix[g, p] = full.T.astype(BF16)

    with scope("w_route"):
        fetch_ids.wait()
        fetch_quanta.wait()
    with scope("tables"):
        tables(route, q, lambda p: True)

    with scope("w_tokens"):
        fetch_tokens.wait()
    for i in range(1, PARTS):
        fetch_split(i).start()
    fetch_in.start()
    fetch_out.start()

    def pack_own(c):
        for p in range(half):
            pack(q, p, lambda i: mine[i], c)

            @pl.when(inner | (q == p))
            def _():
                ship(q, c, p)

    for i in range(PARTS):
        with scope("w_split"):
            fetch_split(i).wait()
        with scope("split"):
            mine[i] = jnp.dot(tokens[...], w_split[i], preferred_element_type=F32).astype(BF16)
        if i == 0:
            with scope("w_barrier"):
                pl.semaphore_wait(barrier, peers - 1 + jnp.where(inner, half, 1))
            info_across().start()

            @pl.when(~inner)
            def _():
                info_near().start()

        @pl.when(~inner | (half == 1) | (i < EARLY))
        def _():
            raw_across(i).start()

        if i % 2 == 1:
            @pl.when(inner)
            def _():
                pack_own(i // 2)

    fetch_merge.start()

    def proxy(g, c):
        for i in (2 * c, 2 * c + 1):
            with scope(f"w_raw{g}"):
                whole(raw.at[g - half, i], raw_recv.at[g - half, i]).wait()
        for p in range(half):
            pack(g, p, lambda i: raw[g - half, i], c)
            ship(g, c, p)

    def ffn(k, g, meanwhile=None):
        for c in range(CHUNKS):
            with scope(f"w_slots{k}"):
                direct = q != jnp.minimum(g, last)

                @pl.when(direct)
                def _():
                    whole(received.at[g, c], slot_recv.at[g, c]).wait()

                @pl.when(jnp.logical_not(direct))
                def _():
                    whole(received.at[g, c, pl.ds(0, n_seq - 1)], slot_recv.at[g, c]).wait()
            with scope("unfold"):
                left, right = unfold(received[g, c])
                x[:, 2 * c * part:(2 * c + 1) * part] = left
                x[:, (2 * c + 1) * part:(2 * c + 2) * part] = right

        if meanwhile is not None:
            meanwhile()
        with scope("gate_up"):
            @pl.loop(0, ffe // TILE)
            def _(t):
                gate_at = pl.ds(pl.multiple_of(t * TILE, TILE), TILE)
                up_at = pl.ds(pl.multiple_of(ffe + t * TILE, TILE), TILE)
                gate = jnp.dot(x[...], w_in[:, gate_at], preferred_element_type=F32)
                up = jnp.dot(x[...], w_in[:, up_at], preferred_element_type=F32)
                hidden[:, gate_at] = (gate / (1.0 + jnp.exp(-gate)) * up).astype(BF16)

        for c in range(CHUNKS):
            with scope("down"):
                y = [jnp.dot(hidden[...], w_out[:, i * part:(i + 1) * part],
                             preferred_element_type=F32).reshape(n_seq, slots, part)
                     for i in (2 * c, 2 * c + 1)]
                answers[g, c] = jnp.concatenate(y, axis=1).astype(BF16)

    def paced(g, c):
        return isinstance(g, int) and g >= half and c < CHUNKS - 1

    def reply_chunk(g, c):
        with scope("reply"):
            @pl.loop(1, n_seq)
            def _(r):
                remote(answers.at[g, c, r], returned.at[g, c, q * n_seq + r],
                       ans_send.at[g, c], ans_recv.at[g, c], near(n_seq - r, q)).start()

            returned[g, c, pl.ds(q * n_seq, 1)] = answers[g, c, 0:1]

    def reply(g):
        for c in range(CHUNKS):
            reply_chunk(g, c)

    def left(g, c):
        with scope("w_left"):
            whole(answers.at[g, c, pl.ds(0, n_seq - 1)], ans_send.at[g, c]).wait()

    def mine_at(g, c, p):
        return returned.at[g, c, pl.ds(p * n_seq, n_seq)]

    def gathered(g, c):
        with scope("w_gather"):
            whole(returned.at[g, c, pl.ds(0, n_seq - 1)], ans_recv.at[g, c]).wait()

    def inward(g, c):
        return remote(mine_at(g, c, q), mine_at(g, c, q), back_send.at[g, c],
                      back_recv.at[g, c, q], (s, plane(side, last)))

    def pass_inward(g, chunks=range(CHUNKS)):
        for c in chunks:
            gathered(g, c)
            inward(g, c).start()

    def combine(g, c, planes, tag):
        gathered(g, c)
        with scope(f"w_reply{tag}"):
            for p in planes:
                if p != last:
                    whole(mine_at(g, c, p), back_recv.at[g, c, p]).wait()
        with scope("combine"):
            total = [None, None]
            for p in planes:
                halves = unfold(returned[g, c, pl.ds(p * n_seq, n_seq)])
                for k in range(2):
                    y = jnp.dot(mix[g, p], halves[k], preferred_element_type=F32)
                    total[k] = y if total[k] is None else total[k] + y
            return total

    every = list(range(half))

    def bring_across(g):
        for c in range(CHUNKS):
            sums = combine(half + g, c, every, half + g)
            for k in range(2):
                part_out[half + g, 2 * c + k] = sums[k].astype(BF16)
                part_across(g, 2 * c + k).start()

    def bring_outward(g):
        for c in range(CHUNKS):
            sums = combine(g, c, [p for p in every if p != g], g)
            for k in range(2):
                i = 2 * c + k
                with scope("w_part"):
                    whole(part_in.at[g, i], part_recv.at[g, i]).wait()
                part_out[g, i] = (sums[k] + part_in[g, i].astype(F32)).astype(BF16)
                part_outward(g, i).start()

    def learn(g):
        with scope("w_info"):
            whole(info.at[g], info_recv.at[g]).wait()
        with scope("tables"):
            tables(info.at[g], g, lambda p: p != g)

    with scope("w_load"):
        fetch_in.wait()
        fetch_out.wait()

    @pl.when(inner)
    def _():
        learn(half)
        proxy(half, 0)
        ffn(0, last)
        for c in range(1, CHUNKS):
            proxy(half, c)
        if half > 1:
            for i in range(EARLY, PARTS):
                raw_across(i).start()
        for g in [*range(half + 1, n_sub), *outers]:
            learn(g)
        for g in range(half + 1, n_sub):
            proxy(g, 0)
            ffn(g - 1, g - 1)
            for c in range(1, CHUNKS):
                proxy(g, c)
            reply(g - 1)
        for g in outers:
            ffn(1 + g, g)
        ffn(n_sub - 1, n_sub - 1)
        for g in outers:
            reply(g)
        reply(n_sub - 1)
        reply(last)
        for g in outers:
            bring_across(g)
        for g in outers:
            bring_outward(g)
        bring_across(last)
        for c in range(CHUNKS):
            sums = combine(last, c, every, "own")
            for k in range(2):
                i = 2 * c + k
                acc[:, i * part:(i + 1) * part] = sums[k]

    @pl.when(~inner)
    def _():
        for c in range(CHUNKS):
            pack_own(c)
        ffn(1, last)
        with scope("w_sent"):
            for i in range(PARTS):
                whole(mine.at[i], raw_send.at[i]).wait()
        for c in range(CHUNKS):
            for p in range(half):
                @pl.when(q != p)
                def _():
                    ship(q, c, p)

        ffn(0, q)
        for g in range(half, n_sub):
            spare = [c for c in range(CHUNKS) if min(c, last) == g - half]

            def meanwhile():
                for c in spare:
                    reply_chunk(last, c)

            ffn(g, g, meanwhile)
            for c in range(CHUNKS):
                reply_chunk(g, c)
                if c == 0:
                    pass_inward(last, spare)
                if paced(g, c):
                    left(g, c)
            pass_inward(g)
        reply(q)

        for g in outers:
            @pl.when(q != g)
            def _():
                ffn(n_sub, g)
                reply(g)
                pass_inward(g)

    for g in outers:
        @pl.when(q == g)
        def _():
            for c in range(CHUNKS):
                gathered(g, c)
                halves = unfold(returned[g, c, pl.ds(g * n_seq, n_seq)])
                for k in range(2):
                    i = 2 * c + k
                    acc[:, i * part:(i + 1) * part] = jnp.dot(
                        mix[g, g], halves[k], preferred_element_type=F32)

    for i in range(PARTS):
        at = slice(i * part, (i + 1) * part)
        with scope("w_part"):
            whole(part_in.at[q, i], part_recv.at[q, i]).wait()
        head[:, at] = (acc[:, at] + part_in[q, i].astype(F32)).astype(BF16)

    with scope("w_merge"):
        fetch_merge.wait()
    tiles = width // TILE

    def target(j):
        y = jnp.where(z < half, z, n_sub - 1 - z)
        far = n_sub - 2 - y
        t = jnp.where(j < far, n_sub - 1 - j, j - far)
        t = jnp.where(j == n_sub - 2, y + 1, jnp.where(j == n_sub - 1, y, t))
        return jnp.where(z < half, t, n_sub - 1 - t)

    def share(t, k):
        cols = pl.ds(pl.multiple_of(t * width + k * TILE, TILE), TILE)
        return jnp.dot(head[...], w_merge[:, cols], preferred_element_type=F32)

    def hop(t, k):
        up = t > z
        to = jnp.where(up, z + 1, z - 1)
        place = jnp.where(up | (t != z - 1), t, n_sub)
        return remote(sending.at[t, k], landed.at[place, k], hop_send.at[t, k],
                      hop_recv.at[place, k], (s, to))

    for j in range(n_sub - 1):
        t = target(j)
        edge = jnp.where(t > z, z == 0, z == n_sub - 1)

        with scope(f"merge{j}"):
            @pl.loop(0, tiles)
            def _(k):
                total = share(t, k)

                @pl.when(edge)
                def _():
                    sending[t, k] = total.astype(BF16)

                @pl.when(~edge)
                def _():
                    whole(landed.at[t, k], hop_recv.at[t, k]).wait()
                    sending[t, k] = (total + landed[t, k].astype(F32)).astype(BF16)

                hop(t, k).start()

    with scope("merge_own"):
        for k in range(tiles):
            acc[:, k * TILE:(k + 1) * TILE] = share(z, k)
    whole(route, info_send.at[1]).wait()

    @pl.when(~inner)
    def _():
        whole(route, info_send.at[0]).wait()

    @pl.when(inner)
    def _():
        for i in range(PARTS):
            whole(mine.at[i], raw_send.at[i]).wait()

    for g in range(n_sub):
        sender = (q == g) | (inner & (g >= half))
        for c in range(CHUNKS):
            @pl.when(inner | (not paced(g, c)))
            def _():
                whole(answers.at[g, c, pl.ds(0, n_seq - 1)], ans_send.at[g, c]).wait()

            @pl.when(~inner & (q != g))
            def _():
                whole(mine_at(g, c, q), back_send.at[g, c]).wait()

            for p in range(half):
                @pl.when(sender & (q == p))
                def _():
                    whole(received.at[g, c, pl.ds(0, n_seq - 1)], slot_send.at[g, c, p]).wait()

                @pl.when(sender & (q != p))
                def _():
                    whole(received.at[g, c], slot_send.at[g, c, p]).wait()

    @pl.when(inner)
    def _():
        for g in range(n_sub):
            for i in range(PARTS):
                if g != last:
                    whole(part_out.at[g, i], part_send.at[g, i]).wait()

    for place, has in ((z, z > 0), (n_sub, z < n_sub - 1)):
        with scope("w_landed"):
            @pl.when(has)
            def _():
                for k in range(tiles):
                    whole(landed.at[place, k], hop_recv.at[place, k]).wait()
                    acc[:, k * TILE:(k + 1) * TILE] += landed[place, k].astype(F32)

    with scope("finish"):
        out[...] = acc[...].astype(out.dtype)

    for t in range(n_sub):
        @pl.when(z != t)
        def _():
            for k in range(tiles):
                whole(sending.at[t, k], hop_send.at[t, k]).wait()


def layer(n_seq, n_sub, slots, ids, quanta, capacity, tokens, w_split, w_in, w_out, w_merge):
    half = n_sub // 2
    rows, width = tokens.shape[0], w_out.shape[1]
    peers, part, tiles = half * n_seq, width // PARTS, width // TILE
    vmem = pl.BlockSpec(memory_space=pltpu.VMEM)
    hbm = pl.BlockSpec(memory_space=pltpu.HBM)

    def buf(*shape, dtype=BF16):
        return pltpu.VMEM(shape, dtype)

    dma = pltpu.SemaphoreType.DMA
    message = (2 * slots, part)
    group = n_seq * slots
    return pl.pallas_call(
        functools.partial(layer_kernel, n_seq, n_sub, slots),
        out_shape=jax.ShapeDtypeStruct((rows, width), BF16),
        in_specs=[hbm] * 2 + [vmem] + [hbm] * 5,
        out_specs=vmem,
        scratch_shapes=[
            buf(*tokens.shape),
            buf(PARTS, w_split.shape[0], part),
            buf(*w_in.shape),
            buf(*w_out.shape),
            buf(*w_merge.shape),
            buf(2, *ids.shape, dtype=jnp.int32),
            buf(n_sub, 2, *ids.shape, dtype=jnp.int32),
            buf(PARTS, rows, part),
            buf(half, PARTS, rows, part),
            buf(n_sub, half, group, rows),
            buf(n_sub, half, rows, group),
            buf(n_sub, CHUNKS, half, n_seq, *message),
            buf(n_sub, CHUNKS, n_seq, *message),
            buf(group, width),
            buf(group, w_out.shape[0]),
            buf(n_sub, CHUNKS, n_seq, *message),
            buf(n_sub, CHUNKS, peers, *message),
            buf(n_sub, PARTS, rows, part),
            buf(half, PARTS, rows, part),
            buf(rows, width, dtype=F32),
            buf(rows, width),
            buf(n_sub, tiles, rows, TILE),
            buf(n_sub + 1, tiles, rows, TILE),
            dma((PARTS + 6,)),
            dma((2,)),
            dma((n_sub,)),
            dma((PARTS,)),
            dma((half, PARTS)),
            dma((n_sub, CHUNKS, half)),
            dma((n_sub, CHUNKS)),
            dma((n_sub, CHUNKS)),
            dma((n_sub, CHUNKS)),
            dma((n_sub, CHUNKS)),
            dma((n_sub, CHUNKS, half)),
            dma((n_sub, PARTS)),
            dma((half, PARTS)),
            dma((n_sub, tiles)),
            dma((n_sub + 1, tiles)),
        ],
        compiler_params=pltpu.CompilerParams(
            collective_id=1, has_side_effects=True, vmem_limit_bytes=VMEM_BYTES),
        name="layer",
    )(ids, quanta, capacity, tokens, w_split, w_in, w_out, w_merge)


def body(n_seq, n_sub, tokens, w_split, w_merge, expert_in, expert_out, expert_ids, combine_q,
         capacity):
    experts = capacity.shape[0]
    slot_count = -(-(3 * tokens.shape[0] // experts) // 8) * 8
    return layer(n_seq, n_sub, slot_count, expert_ids[0].T, combine_q[0].T, capacity[None, :],
                 tokens, w_split, expert_in[0], expert_out[0], w_merge)


def solution(mesh):
    in_specs = (
        P("seq", None),
        P(None, "sub"),
        P("sub", None),
        P(("seq", "sub"), None, None),
        P(("seq", "sub"), None, None),
        P("sub", "seq", None),
        P("sub", "seq", None),
        P(),
    )
    out_specs = P("seq", "sub")
    call = functools.partial(body, mesh.shape["seq"], mesh.shape["sub"])
    return jax.shard_map(call, mesh=mesh, in_specs=in_specs, out_specs=out_specs, check_vma=False)
```

```python
import functools

import jax
import jax.numpy as jnp
from jax import lax
from jax.experimental import pallas as pl
from jax.experimental.pallas import tpu as pltpu
from jax.sharding import PartitionSpec as P

MESH = pl.DeviceIdType.MESH
scope = jax.named_scope
TILE = 256
CHUNKS = 2
PARTS = 2 * CHUNKS
SLABS = 2
EARLY = 1
VMEM_BYTES = 60 * 1024 * 1024
F32 = jnp.float32
BF16 = jnp.bfloat16


def layer_kernel(n_seq, n_sub, slots, ids_hbm, quanta_hbm, capacity, tokens_hbm, w_split_hbm, w_in_hbm,
                 w_out_hbm, w_merge_hbm, out,
                 tokens, w_split, w_in, w_out, w_merge, route, info, mine, raw, pick, mix, packed,
                 received, x, hidden, answers, returned, part_out, part_in, acc, head,
                 sending, landed,
                 load_sem, info_send, info_recv, raw_send, raw_recv, slot_send, slot_recv,
                 ans_send, ans_recv, back_send, back_recv, part_send, part_recv,
                 hop_send, hop_recv):
    s, z = lax.axis_index("seq"), lax.axis_index("sub")
    half = n_sub // 2
    last = half - 1
    side = z // half
    q = jnp.where(side == 0, z, n_sub - 1 - z)
    inner = q == last
    n = n_seq * n_sub
    peers = half * n_seq
    rows, width = acc.shape
    part = width // PARTS
    ffe = w_out.shape[0]
    group = n_seq * slots
    outers = range(last)

    def plane(where, depth):
        return jnp.where(where == 0, depth, n_sub - 1 - depth)

    def near(r, depth):
        return (lax.rem(s + r, n_seq), plane(side, depth))

    def across():
        return (s, plane(1 - side, last))

    deep = tokens.shape[1] // 2

    def fetch_tokens(k):
        at = pl.ds(k * deep, deep)
        return pltpu.make_async_copy(tokens_hbm.at[:, at], tokens.at[:, at],
                                     load_sem.at[(PARTS, PARTS + 6)[k]])

    def fetch_first(k):
        at = pl.ds(k * deep, deep)
        return pltpu.make_async_copy(w_split_hbm.at[at, pl.ds(0, part)], w_split.at[0, at],
                                     load_sem.at[(0, PARTS + 7)[k]])

    fetch_in = pltpu.make_async_copy(w_in_hbm, w_in, load_sem.at[PARTS + 1])
    fetch_out = pltpu.make_async_copy(w_out_hbm, w_out, load_sem.at[PARTS + 2])
    fetch_merge = pltpu.make_async_copy(w_merge_hbm, w_merge, load_sem.at[PARTS + 3])

    def fetch_split(i):
        return pltpu.make_async_copy(
            w_split_hbm.at[:, pl.ds(i * part, part)], w_split.at[i], load_sem.at[i])

    fetch_ids = pltpu.make_async_copy(ids_hbm, route.at[0], load_sem.at[PARTS + 4])
    fetch_quanta = pltpu.make_async_copy(quanta_hbm, route.at[1], load_sem.at[PARTS + 5])
    fetch_ids.start()
    fetch_quanta.start()
    for k in range(2):
        fetch_tokens(k).start()
        fetch_first(k).start()

    barrier = pltpu.get_barrier_semaphore()
    for p in range(half):
        @pl.loop(0, n_seq)
        def _(r):
            @pl.when((r != 0) | (q != p))
            def _():
                pl.semaphore_signal(barrier, inc=1, device_id=near(r, p), device_id_type=MESH)

        @pl.when(inner | (p == last))
        def _():
            pl.semaphore_signal(barrier, inc=1, device_id=(s, plane(1 - side, p)),
                                device_id_type=MESH)

    def remote(src, dst, send, recv, to):
        return pltpu.make_async_remote_copy(src_ref=src, dst_ref=dst, send_sem=send,
                                            recv_sem=recv, device_id=to, device_id_type=MESH)

    def whole(ref, sem):
        return pltpu.make_async_copy(ref, ref, sem)

    def info_near():
        return remote(route, info.at[q], info_send.at[0], info_recv.at[q], (s, plane(side, last)))

    def info_across():
        return remote(route, info.at[half + q], info_send.at[1], info_recv.at[half + q], across())

    def raw_across(i):
        return remote(mine.at[i], raw.at[q, i], raw_send.at[i], raw_recv.at[q, i], across())

    def slab(b):
        return pl.ds(b * (rows // SLABS), rows // SLABS)

    def part_across(g, i, b):
        return remote(part_out.at[half + g, i, slab(b)], part_in.at[g, i, slab(b)],
                      part_send.at[half + g, i, b], part_recv.at[g, i, b], across())

    def part_outward(g, i, b):
        return remote(part_out.at[g, i, slab(b)], part_in.at[g, i, slab(b)],
                      part_send.at[g, i, b], part_recv.at[g, i, b], (s, plane(side, g)))

    def part_arrived(g, i, b):
        with scope("w_part"):
            whole(part_in.at[g, i, slab(b)], part_recv.at[g, i, b]).wait()

    def ship(g, c, p):
        with scope("ship"):
            @pl.loop(0, n_seq)
            def _(r):
                @pl.when((r != 0) | (q != p))
                def _():
                    remote(packed.at[g, c, p, r], received.at[g, c, r], slot_send.at[g, c, p],
                           slot_recv.at[g, c], near(r, p)).start()

            @pl.when(q == p)
            def _():
                received[g, c, 0:1] = packed[g, c, p, 0:1]

    def unfold(y):
        y = y.astype(F32)
        return (y[:, :slots].reshape(group, part).astype(BF16),
                y[:, slots:].reshape(group, part).astype(BF16))

    def pack(g, p, block, c):
        with scope("pack"):
            y = [jnp.dot(pick[g, p], block(2 * c + k), preferred_element_type=F32)
                 .reshape(n_seq, slots, part) for k in range(2)]
            packed[g, c, p] = jnp.concatenate(y, axis=1).astype(BF16)

    square = lax.broadcasted_iota(jnp.int32, (n, n), 0)
    cross = lax.broadcasted_iota(jnp.int32, (n, n), 1)
    limit = jnp.sum(jnp.where(square == cross, capacity[...].astype(F32), 0.0),
                    axis=1, keepdims=True)
    expert = lax.broadcasted_iota(jnp.int32, (n, 1), 0).astype(F32)
    expert_seq = jnp.floor((expert + 0.5) / n_sub)
    expert_sub = (expert - expert_seq * n_sub).astype(jnp.int32)
    away = expert_seq.astype(jnp.int32) - s
    away = jnp.where(away < 0, away + n_seq, away)
    depth = jnp.where(side == 0, expert_sub, n_sub - 1 - expert_sub)
    seats = jnp.where(depth < half, (depth * n_seq + away) * slots, -1).astype(F32)

    def tables(ids, g, wanted):
        places = lax.broadcasted_iota(jnp.int32, (n, rows), 0)
        named = [(places == ids[0, k:k + 1, :]).astype(F32) for k in range(2)]
        before = (lax.broadcasted_iota(jnp.int32, (rows, rows), 0)
                  < lax.broadcasted_iota(jnp.int32, (rows, rows), 1))
        earlier = jnp.dot((named[0] + named[1]).astype(BF16), before.astype(F32).astype(BF16),
                          preferred_element_type=F32)
        slot, weight = [], []
        for k in range(2):
            rank = jnp.sum(named[k] * earlier, axis=0, keepdims=True)
            most = jnp.sum(named[k] * limit, axis=0, keepdims=True)
            seat = jnp.sum(named[k] * seats, axis=0, keepdims=True)
            kept = (rank < most) & (seat >= 0.0)
            slot.append(jnp.where(kept, seat + rank, -1.0).astype(jnp.int32))
            weight.append(ids[1, k:k + 1, :].astype(F32) / 65536.0)
        for p in range(half):
            if wanted(p):
                at = lax.broadcasted_iota(jnp.int32, (group, rows), 0) + p * group
                first, second = at == slot[0], at == slot[1]
                pick[g, p] = (jnp.where(first, 1.0, 0.0) + jnp.where(second, 1.0, 0.0)).astype(BF16)
                full = jnp.where(first, weight[0], 0.0) + jnp.where(second, weight[1], 0.0)
                mix[g, p] = full.T.astype(BF16)

    with scope("w_route"):
        fetch_ids.wait()
        fetch_quanta.wait()
    with scope("tables"):
        tables(route, q, lambda p: True)

    for i in range(1, PARTS):
        fetch_split(i).start()
    fetch_in.start()
    fetch_out.start()

    def pack_own(c):
        for p in range(half):
            pack(q, p, lambda i: mine[i], c)

            @pl.when(inner | (q == p))
            def _():
                ship(q, c, p)

    for i in range(PARTS):
        if i == 0:
            total = None
            for k in range(2):
                with scope("w_split"):
                    fetch_tokens(k).wait()
                    fetch_first(k).wait()
                at = slice(k * deep, (k + 1) * deep)
                y = jnp.dot(tokens[:, at], w_split[0, at], preferred_element_type=F32)
                total = y if total is None else total + y
            mine[0] = total.astype(BF16)
        else:
            with scope("w_split"):
                fetch_split(i).wait()
            with scope("split"):
                mine[i] = jnp.dot(tokens[...], w_split[i],
                                  preferred_element_type=F32).astype(BF16)
        if i == 0:
            with scope("w_barrier"):
                pl.semaphore_wait(barrier, peers - 1 + jnp.where(inner, half, 1))
            info_across().start()

            @pl.when(~inner)
            def _():
                info_near().start()

        @pl.when(~inner | (half == 1) | (i < EARLY))
        def _():
            raw_across(i).start()

        if i % 2 == 1:
            @pl.when(inner)
            def _():
                pack_own(i // 2)

    fetch_merge.start()

    def proxy(g, c):
        for i in (2 * c, 2 * c + 1):
            with scope(f"w_raw{g}"):
                whole(raw.at[g - half, i], raw_recv.at[g - half, i]).wait()
        for p in range(half):
            pack(g, p, lambda i: raw[g - half, i], c)
            ship(g, c, p)

    def ffn(k, g, meanwhile=None):
        for c in range(CHUNKS):
            with scope(f"w_slots{k}"):
                direct = q != jnp.minimum(g, last)

                @pl.when(direct)
                def _():
                    whole(received.at[g, c], slot_recv.at[g, c]).wait()

                @pl.when(jnp.logical_not(direct))
                def _():
                    whole(received.at[g, c, pl.ds(0, n_seq - 1)], slot_recv.at[g, c]).wait()
            with scope("unfold"):
                left, right = unfold(received[g, c])
                x[:, 2 * c * part:(2 * c + 1) * part] = left
                x[:, (2 * c + 1) * part:(2 * c + 2) * part] = right

        if meanwhile is not None:
            meanwhile()
        with scope("gate_up"):
            @pl.loop(0, ffe // TILE)
            def _(t):
                gate_at = pl.ds(pl.multiple_of(t * TILE, TILE), TILE)
                up_at = pl.ds(pl.multiple_of(ffe + t * TILE, TILE), TILE)
                gate = jnp.dot(x[...], w_in[:, gate_at], preferred_element_type=F32)
                up = jnp.dot(x[...], w_in[:, up_at], preferred_element_type=F32)
                hidden[:, gate_at] = (gate / (1.0 + jnp.exp(-gate)) * up).astype(BF16)

        for c in range(CHUNKS):
            with scope("down"):
                y = [jnp.dot(hidden[...], w_out[:, i * part:(i + 1) * part],
                             preferred_element_type=F32).reshape(n_seq, slots, part)
                     for i in (2 * c, 2 * c + 1)]
                answers[g, c] = jnp.concatenate(y, axis=1).astype(BF16)

    def paced(g, c):
        return isinstance(g, int) and g >= half and c < CHUNKS - 1

    def reply_chunk(g, c):
        with scope("reply"):
            @pl.loop(1, n_seq)
            def _(r):
                remote(answers.at[g, c, r], returned.at[g, c, q * n_seq + r],
                       ans_send.at[g, c], ans_recv.at[g, c], near(n_seq - r, q)).start()

            returned[g, c, pl.ds(q * n_seq, 1)] = answers[g, c, 0:1]

    def reply(g):
        for c in range(CHUNKS):
            reply_chunk(g, c)

    def left(g, c):
        with scope("w_left"):
            whole(answers.at[g, c, pl.ds(0, n_seq - 1)], ans_send.at[g, c]).wait()

    def mine_at(g, c, p):
        return returned.at[g, c, pl.ds(p * n_seq, n_seq)]

    def gathered(g, c):
        with scope("w_gather"):
            whole(returned.at[g, c, pl.ds(0, n_seq - 1)], ans_recv.at[g, c]).wait()

    def inward(g, c):
        return remote(mine_at(g, c, q), mine_at(g, c, q), back_send.at[g, c],
                      back_recv.at[g, c, q], (s, plane(side, last)))

    def pass_inward(g, chunks=range(CHUNKS)):
        for c in chunks:
            gathered(g, c)
            inward(g, c).start()

    def combine(g, c, planes, tag):
        gathered(g, c)
        with scope(f"w_reply{tag}"):
            for p in planes:
                if p != last:
                    whole(mine_at(g, c, p), back_recv.at[g, c, p]).wait()
        with scope("combine"):
            total = [None, None]
            for p in planes:
                halves = unfold(returned[g, c, pl.ds(p * n_seq, n_seq)])
                for k in range(2):
                    y = jnp.dot(mix[g, p], halves[k], preferred_element_type=F32)
                    total[k] = y if total[k] is None else total[k] + y
            return total

    every = list(range(half))

    def bring_across(g):
        for c in range(CHUNKS):
            sums = combine(half + g, c, every, half + g)
            for k in range(2):
                part_out[half + g, 2 * c + k] = sums[k].astype(BF16)
                for b in range(SLABS):
                    part_across(g, 2 * c + k, b).start()

    def bring_outward(g):
        for c in range(CHUNKS):
            sums = combine(g, c, [p for p in every if p != g], g)
            for k in range(2):
                i = 2 * c + k
                for b in range(SLABS):
                    part_arrived(g, i, b)
                    at = slice(b * (rows // SLABS), (b + 1) * (rows // SLABS))
                    part_out[g, i, at] = (sums[k][at] + part_in[g, i, at].astype(F32)).astype(BF16)
                    part_outward(g, i, b).start()

    def learn(g):
        with scope("w_info"):
            whole(info.at[g], info_recv.at[g]).wait()
        with scope("tables"):
            tables(info.at[g], g, lambda p: p != g)

    with scope("w_load"):
        fetch_in.wait()
        fetch_out.wait()

    @pl.when(inner)
    def _():
        learn(half)
        proxy(half, 0)
        ffn(0, last)
        for c in range(1, CHUNKS):
            proxy(half, c)
        if half > 1:
            for i in range(EARLY, PARTS):
                raw_across(i).start()
        for g in [*range(half + 1, n_sub), *outers]:
            learn(g)
        for g in range(half + 1, n_sub):
            proxy(g, 0)
            ffn(g - 1, g - 1)
            for c in range(1, CHUNKS):
                proxy(g, c)
            reply(g - 1)
        for g in outers:
            ffn(1 + g, g)
        ffn(n_sub - 1, n_sub - 1)
        for g in outers:
            reply(g)
        reply(n_sub - 1)
        reply(last)
        for g in outers:
            bring_across(g)
        for g in outers:
            bring_outward(g)
        bring_across(last)
        for c in range(CHUNKS):
            sums = combine(last, c, every, "own")
            for k in range(2):
                i = 2 * c + k
                acc[:, i * part:(i + 1) * part] = sums[k]

    @pl.when(~inner)
    def _():
        for c in range(CHUNKS):
            pack_own(c)
        ffn(1, last)
        with scope("w_sent"):
            for i in range(PARTS):
                whole(mine.at[i], raw_send.at[i]).wait()
        for c in range(CHUNKS):
            for p in range(half):
                @pl.when(q != p)
                def _():
                    ship(q, c, p)

        ffn(0, q)
        rest = range(1, CHUNKS)
        reply_chunk(last, 0)

        def meanwhile():
            for c in rest:
                reply_chunk(last, c)

        for g in range(half, n_sub):
            ffn(g, g, meanwhile if g == n_sub - 1 else None)
            for c in range(CHUNKS):
                reply_chunk(g, c)
                if g == half and c == 0:
                    pass_inward(last, [0])
                if paced(g, c):
                    left(g, c)
            pass_inward(g)
        pass_inward(last, rest)
        reply(q)

        for g in outers:
            @pl.when(q != g)
            def _():
                ffn(n_sub, g)
                reply(g)
                pass_inward(g)

    for g in outers:
        @pl.when(q == g)
        def _():
            for c in range(CHUNKS):
                gathered(g, c)
                halves = unfold(returned[g, c, pl.ds(g * n_seq, n_seq)])
                for k in range(2):
                    i = 2 * c + k
                    acc[:, i * part:(i + 1) * part] = jnp.dot(
                        mix[g, g], halves[k], preferred_element_type=F32)

    for i in range(PARTS):
        at = slice(i * part, (i + 1) * part)
        for b in range(SLABS):
            part_arrived(q, i, b)
        head[:, at] = (acc[:, at] + part_in[q, i].astype(F32)).astype(BF16)

    with scope("w_merge"):
        fetch_merge.wait()
    tiles = width // TILE

    def target(j):
        y = jnp.where(z < half, z, n_sub - 1 - z)
        far = n_sub - 2 - y
        t = jnp.where(j < far, n_sub - 1 - j, j - far)
        t = jnp.where(j == n_sub - 2, y + 1, jnp.where(j == n_sub - 1, y, t))
        return jnp.where(z < half, t, n_sub - 1 - t)

    def share(t, k):
        cols = pl.ds(pl.multiple_of(t * width + k * TILE, TILE), TILE)
        return jnp.dot(head[...], w_merge[:, cols], preferred_element_type=F32)

    def hop(t, k):
        up = t > z
        to = jnp.where(up, z + 1, z - 1)
        place = jnp.where(up | (t != z - 1), t, n_sub)
        return remote(sending.at[t, k], landed.at[place, k], hop_send.at[t, k],
                      hop_recv.at[place, k], (s, to))

    for j in range(n_sub - 1):
        t = target(j)
        edge = jnp.where(t > z, z == 0, z == n_sub - 1)

        with scope(f"merge{j}"):
            @pl.loop(0, tiles)
            def _(k):
                total = share(t, k)

                @pl.when(edge)
                def _():
                    sending[t, k] = total.astype(BF16)

                @pl.when(~edge)
                def _():
                    whole(landed.at[t, k], hop_recv.at[t, k]).wait()
                    sending[t, k] = (total + landed[t, k].astype(F32)).astype(BF16)

                hop(t, k).start()

    with scope("merge_own"):
        for k in range(tiles):
            acc[:, k * TILE:(k + 1) * TILE] = share(z, k)
    whole(route, info_send.at[1]).wait()

    @pl.when(~inner)
    def _():
        whole(route, info_send.at[0]).wait()

    @pl.when(inner)
    def _():
        for i in range(PARTS):
            whole(mine.at[i], raw_send.at[i]).wait()

    for g in range(n_sub):
        sender = (q == g) | (inner & (g >= half))
        for c in range(CHUNKS):
            @pl.when(inner | (not paced(g, c)))
            def _():
                whole(answers.at[g, c, pl.ds(0, n_seq - 1)], ans_send.at[g, c]).wait()

            @pl.when(~inner & (q != g))
            def _():
                whole(mine_at(g, c, q), back_send.at[g, c]).wait()

            for p in range(half):
                @pl.when(sender & (q == p))
                def _():
                    whole(received.at[g, c, pl.ds(0, n_seq - 1)], slot_send.at[g, c, p]).wait()

                @pl.when(sender & (q != p))
                def _():
                    whole(received.at[g, c], slot_send.at[g, c, p]).wait()

    @pl.when(inner)
    def _():
        for g in range(n_sub):
            for i in range(PARTS):
                if g != last:
                    for b in range(SLABS):
                        whole(part_out.at[g, i, slab(b)], part_send.at[g, i, b]).wait()

    for place, has in ((z, z > 0), (n_sub, z < n_sub - 1)):
        with scope("w_landed"):
            @pl.when(has)
            def _():
                for k in range(tiles):
                    whole(landed.at[place, k], hop_recv.at[place, k]).wait()
                    acc[:, k * TILE:(k + 1) * TILE] += landed[place, k].astype(F32)

    with scope("finish"):
        out[...] = acc[...].astype(out.dtype)

    for t in range(n_sub):
        @pl.when(z != t)
        def _():
            for k in range(tiles):
                whole(sending.at[t, k], hop_send.at[t, k]).wait()


def layer(n_seq, n_sub, slots, ids, quanta, capacity, tokens, w_split, w_in, w_out, w_merge):
    half = n_sub // 2
    rows, width = tokens.shape[0], w_out.shape[1]
    peers, part, tiles = half * n_seq, width // PARTS, width // TILE
    vmem = pl.BlockSpec(memory_space=pltpu.VMEM)
    hbm = pl.BlockSpec(memory_space=pltpu.HBM)

    def buf(*shape, dtype=BF16):
        return pltpu.VMEM(shape, dtype)

    dma = pltpu.SemaphoreType.DMA
    message = (2 * slots, part)
    group = n_seq * slots
    return pl.pallas_call(
        functools.partial(layer_kernel, n_seq, n_sub, slots),
        out_shape=jax.ShapeDtypeStruct((rows, width), BF16),
        in_specs=[hbm] * 2 + [vmem] + [hbm] * 5,
        out_specs=vmem,
        scratch_shapes=[
            buf(*tokens.shape),
            buf(PARTS, w_split.shape[0], part),
            buf(*w_in.shape),
            buf(*w_out.shape),
            buf(*w_merge.shape),
            buf(2, *ids.shape, dtype=jnp.int32),
            buf(n_sub, 2, *ids.shape, dtype=jnp.int32),
            buf(PARTS, rows, part),
            buf(half, PARTS, rows, part),
            buf(n_sub, half, group, rows),
            buf(n_sub, half, rows, group),
            buf(n_sub, CHUNKS, half, n_seq, *message),
            buf(n_sub, CHUNKS, n_seq, *message),
            buf(group, width),
            buf(group, w_out.shape[0]),
            buf(n_sub, CHUNKS, n_seq, *message),
            buf(n_sub, CHUNKS, peers, *message),
            buf(n_sub, PARTS, rows, part),
            buf(half, PARTS, rows, part),
            buf(rows, width, dtype=F32),
            buf(rows, width),
            buf(n_sub, tiles, rows, TILE),
            buf(n_sub + 1, tiles, rows, TILE),
            dma((PARTS + 8,)),
            dma((2,)),
            dma((n_sub,)),
            dma((PARTS,)),
            dma((half, PARTS)),
            dma((n_sub, CHUNKS, half)),
            dma((n_sub, CHUNKS)),
            dma((n_sub, CHUNKS)),
            dma((n_sub, CHUNKS)),
            dma((n_sub, CHUNKS)),
            dma((n_sub, CHUNKS, half)),
            dma((n_sub, PARTS, SLABS)),
            dma((half, PARTS, SLABS)),
            dma((n_sub, tiles)),
            dma((n_sub + 1, tiles)),
        ],
        compiler_params=pltpu.CompilerParams(
            collective_id=1, has_side_effects=True, vmem_limit_bytes=VMEM_BYTES),
        name="layer",
    )(ids, quanta, capacity, tokens, w_split, w_in, w_out, w_merge)


def body(n_seq, n_sub, tokens, w_split, w_merge, expert_in, expert_out, expert_ids, combine_q,
         capacity):
    experts = capacity.shape[0]
    slot_count = -(-(3 * tokens.shape[0] // experts) // 8) * 8
    return layer(n_seq, n_sub, slot_count, expert_ids[0].T, combine_q[0].T, capacity[None, :],
                 tokens, w_split, expert_in[0], expert_out[0], w_merge)


def solution(mesh):
    in_specs = (
        P("seq", None),
        P(None, "sub"),
        P("sub", None),
        P(("seq", "sub"), None, None),
        P(("seq", "sub"), None, None),
        P("sub", "seq", None),
        P("sub", "seq", None),
        P(),
    )
    out_specs = P("seq", "sub")
    call = functools.partial(body, mesh.shape["seq"], mesh.shape["sub"])
    return jax.shard_map(call, mesh=mesh, in_specs=in_specs, out_specs=out_specs, check_vma=False)
```
